32 devices in a mesh: row: 4 (over y, x), col: 8 (over z, core).
Axes of the slice: x: 2, y: 2, z: 4, core: 2. Of those that a mesh axis runs over, the one named last changes fastest.
Arguments:
- samples: bfloat16 [8, 4, 256, 16384], P('col', 'row'), may hold values from -6 to 6
- w_start: float32 [32768, 256], P(('row', 'col')), may hold values from 0.005 to 2
- h_start: float32 [256, 2048], P('row', 'col'), may hold values from 0.005 to 2
Outputs:
- w_final: float32 [32768, 256], P(('row', 'col'))
- h_final: float32 [256, 2048], P('row', 'col')
The draws below stay inside these ranges and needn't reach their ends.
All inputs are finite; a program needn't handle non-finite values.
Results may differ from the reference program's by a relative error of at most 0.0013.
Values may be sent and summed in bfloat16 or wider, within the bound.
A program may use at most 128 MiB of HBM per device.

```python
import math
import jax
import jax.numpy as jnp
from jax import lax

CH = 256
BINS = 128
RANK = 256
FR = 64
ITERS = 2
WIN = 256
CHB = 32768
FRAMES = 2048
N_ROW = 4
N_COL = 8


def draw_samples(key, part):
    subkeys = [jax.random.fold_in(key, 101 + index) for index in range(7)]
    full_shape = (N_COL, N_ROW, CH, FR, WIN)
    white_noise = jax.random.normal(subkeys[0], full_shape, jnp.float32)
    block_level = jax.random.uniform(subkeys[1], (N_COL, N_ROW, CH, 1, 1), jnp.float32, -0.9, 0.9)
    frame_level = jax.random.uniform(subkeys[2], (N_COL, N_ROW, CH, FR, 1), jnp.float32, -0.6, 0.6)
    tone_bins = jax.random.randint(subkeys[3], (CH, 3), 1, BINS).astype(jnp.int32)
    amplitude = jax.random.uniform(subkeys[4], (CH, 3, 1), jnp.float32, 0.3, 1.0)
    offset = jax.random.uniform(subkeys[5], (CH, 3, 1), jnp.float32, -math.pi, math.pi)
    sample_idx = jnp.arange(WIN, dtype=jnp.int32)
    phase_steps = tone_bins[:, :, None] * sample_idx[None, None, :] % WIN
    tone_wave = jnp.sum(amplitude * jnp.cos(phase_steps.astype(jnp.float32) * (2.0 * math.pi / WIN) + offset), axis=1)
    tone_level = jnp.exp(jax.random.uniform(subkeys[6], (N_COL, N_ROW, CH, 1, 1), jnp.float32, -1.0, 1.0))
    values = white_noise * jnp.exp(block_level + frame_level) + tone_level * tone_wave[None, None, :, None, :]
    values = jnp.clip(values, -6.0, 6.0)
    return values.reshape(N_COL, N_ROW, CH, FR * WIN).astype(jnp.bfloat16)


def draw_w_start(key, part):
    base_key = jax.random.fold_in(key, 201)
    choose_key = jax.random.fold_in(key, 202)
    base = jnp.exp(jax.random.uniform(base_key, (CHB, RANK), jnp.float32, math.log(0.01), math.log(0.1)))
    boost = 20.0
    chosen = jax.random.randint(choose_key, (CH, 1, RANK), 0, 16) == 0
    favour = jnp.broadcast_to(jnp.where(chosen, boost, 1.0).astype(jnp.float32), (CH, BINS, RANK)).reshape(CHB, RANK)
    return (base * favour).astype(jnp.float32)


def draw_h_start(key, part):
    base_key = jax.random.fold_in(key, 301)
    choose_key = jax.random.fold_in(key, 302)
    base = jnp.exp(jax.random.uniform(base_key, (RANK, FRAMES), jnp.float32, math.log(0.01), math.log(0.1)))
    boost = 20.0
    block_count = FRAMES // FR
    chosen = jax.random.randint(choose_key, (RANK, block_count, 1), 0, 16) == 0
    favour = jnp.broadcast_to(jnp.where(chosen, boost, 1.0).astype(jnp.float32), (RANK, block_count, FR)).reshape(RANK, FRAMES)
    return (base * favour).astype(jnp.float32)


def setup_inputs(seed: int = 0) -> dict:
    splits = jax.random.split(jax.random.key(seed), 4)
    samples = draw_samples(jax.random.fold_in(splits[3], 71), 0)
    w_start = draw_w_start(jax.random.fold_in(splits[3], 71), 0)
    h_start = draw_h_start(jax.random.fold_in(splits[3], 71), 0)
    return {"samples": samples, "w_start": w_start, "h_start": h_start}


def dft_table():
    sample_idx = jnp.arange(WIN, dtype=jnp.int32)
    bin_idx = jnp.arange(BINS, dtype=jnp.int32)
    phases = sample_idx[:, None] * bin_idx[None, :] % WIN
    phases = phases.astype(jnp.float32) * (2.0 * math.pi / WIN)
    shaping = 0.5 - 0.5 * jnp.cos(sample_idx.astype(jnp.float32) * (2.0 * math.pi / WIN))
    shaping = shaping / math.sqrt(3.0 * WIN / 8.0)
    both = jnp.concatenate([shaping[:, None] * jnp.cos(phases), -shaping[:, None] * jnp.sin(phases)], axis=1)
    return both.astype(jnp.bfloat16)

def reference(samples, w_start, h_start):
    table = dft_table()
    record = samples.transpose(2, 0, 1, 3).reshape(CH, FRAMES, WIN)

    def channel_energy(trace):
        spectrum = jnp.dot(trace, table, preferred_element_type=jnp.float32)
        real_part = spectrum[:, :BINS]
        imag_part = spectrum[:, BINS:]
        return (real_part * real_part + imag_part * imag_part).astype(jnp.bfloat16)
    energy = lax.map(channel_energy, record)
    spectra = energy.transpose(0, 2, 1).reshape(CHB, FRAMES)
    block_rows = CHB // N_ROW
    spectra_blocks = spectra.reshape(N_ROW, block_rows, FRAMES)
    w_state = w_start
    h_state = h_start
    for sweep in range(ITERS):
        w_b = w_state.astype(jnp.bfloat16)
        h_b = h_state.astype(jnp.bfloat16)

        def block_step(running, inputs):
            spectra_part, w_part = inputs
            recon = jnp.dot(w_part, h_b, preferred_element_type=jnp.float32)
            quotient = (spectra_part / recon).astype(jnp.bfloat16)
            h_add = jnp.dot(w_part.T, quotient, preferred_element_type=jnp.float32)
            w_part_numer = jnp.dot(quotient, h_b.T, preferred_element_type=jnp.float32)
            return (running + h_add, w_part_numer)
        h_numer, w_numer = lax.scan(block_step, jnp.zeros((RANK, FRAMES), jnp.float32), (spectra_blocks, w_b.reshape(N_ROW, block_rows, RANK)))
        w_numer = w_numer.reshape(CHB, RANK)
        w_colsum = lax.optimization_barrier(jnp.sum(w_b.astype(jnp.float32), axis=0))
        h_rowsum = lax.optimization_barrier(jnp.sum(h_b.astype(jnp.float32), axis=1))
        h_state = h_state * h_numer / w_colsum[:, None]
        w_state = w_state * w_numer / h_rowsum[None, :]
    return (w_state, h_state)
```

```python
import functools
import math

import jax
import jax.numpy as jnp
from jax import lax
from jax.experimental import pallas as pl
from jax.experimental.pallas import tpu as pltpu
from jax.sharding import PartitionSpec as P

BINS = 128
ITERS = 2
WIN = 256


def dft_table():
    sample_idx = jnp.arange(WIN, dtype=jnp.int32)
    bin_idx = jnp.arange(BINS, dtype=jnp.int32)
    phases = sample_idx[:, None] * bin_idx[None, :] % WIN
    phases = phases.astype(jnp.float32) * (2.0 * math.pi / WIN)
    shaping = 0.5 - 0.5 * jnp.cos(sample_idx.astype(jnp.float32) * (2.0 * math.pi / WIN))
    shaping = shaping / math.sqrt(3.0 * WIN / 8.0)
    both = jnp.concatenate(
        [shaping[:, None] * jnp.cos(phases), -shaping[:, None] * jnp.sin(phases)], axis=1
    )
    return both.astype(jnp.bfloat16)


MESH = pl.DeviceIdType.MESH


def greet(partners):
    barrier = pltpu.get_barrier_semaphore()
    for row, col in partners:
        pl.semaphore_signal(barrier, inc=1, device_id={"row": row, "col": col}, device_id_type=MESH)
    pl.semaphore_wait(barrier, len(partners))


class Gather:
    def __init__(self, n_row, n_col, out, sends, recvs):
        self.n_row, self.n_col = n_row, n_col
        self.row, self.col = lax.axis_index("row"), lax.axis_index("col")
        self.core, self.chip = lax.rem(self.col, 2), self.col // 2
        self.chips = n_col // 2
        self.out, self.sends, self.recvs = out, sends, recvs

    def chip_partner(self, k):
        return self.row, lax.rem(self.chip + k, self.chips) * 2 + self.core

    def row_partner(self, k):
        return lax.rem(self.row + k, self.n_row), self.col

    def core_partner(self):
        return self.row, self.chip * 2 + 1 - self.core

    def partners(self):
        chips = [self.chip_partner(k) for k in range(1, self.chips)]
        rows = [self.row_partner(k) for k in range(1, self.n_row)]
        return chips + rows + [self.core_partner()]

    def copy(self, src, dst, index, partner):
        return pltpu.make_async_remote_copy(
            src_ref=src,
            dst_ref=dst,
            send_sem=self.sends.at[index],
            recv_sem=self.recvs.at[index],
            device_id={"row": partner[0], "col": partner[1]},
            device_id_type=MESH,
        )

    def chip_copies(self):
        slot = self.out.at[self.row, self.core, self.chip]
        return [self.copy(slot, slot, k - 1, self.chip_partner(k)) for k in range(1, self.chips)]

    def row_copies(self):
        slot = self.out.at[self.row, self.core]
        base = self.chips - 2
        return [self.copy(slot, slot, base + k, self.row_partner(k)) for k in range(1, self.n_row)]

    def core_copies(self):
        base = self.chips + self.n_row - 2
        slots = [self.out.at[r, self.core] for r in range(self.n_row)]
        return [self.copy(s, s, base + r, self.core_partner()) for r, s in enumerate(slots)]

    def place(self, mine):
        self.out[self.row, self.core, self.chip] = mine[...]

    def stage(self, number):
        lists = (self.chip_copies, self.row_copies, self.core_copies)
        if number > 0:
            for copy in lists[number - 1]():
                copy.wait()
        if number < 3:
            for copy in lists[number]():
                copy.start()


def gather_scratch(n_row, n_col, h_b):
    sems = pltpu.SemaphoreType.DMA((n_col // 2 + 2 * n_row,))
    return [pltpu.VMEM((n_row, 2, n_col // 2, *h_b.shape), h_b.dtype), sems, sems]


def gather_kernel(n_row, n_col, h_ref, out_ref, held, sends, recvs):
    gather = Gather(n_row, n_col, held, sends, recvs)
    gather.place(h_ref)
    greet(gather.partners())
    for number in range(4):
        gather.stage(number)
    out_ref[...] = held[...]


def gather_factor(n_row, n_col, h_b):
    return pl.pallas_call(
        functools.partial(gather_kernel, n_row, n_col),
        in_specs=[pl.BlockSpec(memory_space=pltpu.VMEM)],
        out_specs=pl.BlockSpec(memory_space=pltpu.VMEM),
        out_shape=jax.ShapeDtypeStruct((n_row, 2, n_col // 2, *h_b.shape), h_b.dtype),
        scratch_shapes=gather_scratch(n_row, n_col, h_b),
        compiler_params=pltpu.CompilerParams(collective_id=2, has_side_effects=True),
        name="gather_factor",
    )(h_b)


def exchange_kernel(n_row, n_col, x_ref, out_ref, sends, recvs, own_sem):
    n = n_row * n_col
    row, col = lax.axis_index("row"), lax.axis_index("col")
    me = row * n_col + col
    barrier = pltpu.get_barrier_semaphore()

    def partner(k):
        to_row = lax.rem(row + lax.rem(k, n_row), n_row)
        to_col = lax.rem(col + k // n_row, n_col)
        return to_row, to_col

    def signal(k, carry):
        to_row, to_col = partner(k)
        pl.semaphore_signal(
            barrier, inc=1, device_id={"row": to_row, "col": to_col}, device_id_type=MESH
        )
        return carry

    def copy(k):
        to_row, to_col = partner(k)
        return pltpu.make_async_remote_copy(
            src_ref=x_ref.at[to_row * n_col + to_col],
            dst_ref=out_ref.at[me],
            send_sem=sends.at[k],
            recv_sem=recvs.at[k],
            device_id={"row": to_row, "col": to_col},
            device_id_type=MESH,
        )

    def start(k, carry):
        copy(k).start()
        return carry

    def finish(k, carry):
        copy(k).wait()
        return carry

    own = pltpu.make_async_copy(x_ref.at[me], out_ref.at[me], own_sem)
    own.start()
    lax.fori_loop(1, n, signal, 0)
    pl.semaphore_wait(barrier, n - 1)
    lax.fori_loop(1, n, start, 0)
    lax.fori_loop(1, n, finish, 0)
    own.wait()


def exchange(n_row, n_col, x, space, number, name):
    n = n_row * n_col
    return pl.pallas_call(
        functools.partial(exchange_kernel, n_row, n_col),
        in_specs=[pl.BlockSpec(memory_space=space)],
        out_specs=pl.BlockSpec(memory_space=space),
        out_shape=jax.ShapeDtypeStruct(x.shape, x.dtype),
        scratch_shapes=[
            pltpu.SemaphoreType.DMA((n,)),
            pltpu.SemaphoreType.DMA((n,)),
            pltpu.SemaphoreType.DMA,
        ],
        compiler_params=pltpu.CompilerParams(collective_id=number, has_side_effects=True),
        name=name,
    )(x)


def reduce_kernel(
    n_row, n_col, x_ref, out_ref, pair, summed, row_landed, second, chip_landed, sends, recvs
):
    row, col = lax.axis_index("row"), lax.axis_index("col")
    core, chip = lax.rem(col, 2), col // 2
    chips = n_col // 2

    def row_at(k):
        return lax.rem(row + k, n_row)

    def chip_at(k):
        return lax.rem(chip + k, chips)

    mate = (row, chip * 2 + 1 - core)
    greet(
        [mate]
        + [(row_at(k), col) for k in range(1, n_row)]
        + [(row, chip_at(k) * 2 + core) for k in range(1, chips)]
    )

    def copy(src, dst, index, partner):
        return pltpu.make_async_remote_copy(
            src_ref=src,
            dst_ref=dst,
            send_sem=sends.at[index],
            recv_sem=recvs.at[index],
            device_id={"row": partner[0], "col": partner[1]},
            device_id_type=MESH,
        )

    swaps = [copy(x_ref.at[1 - core, row_at(k)], pair.at[k], k, mate) for k in range(n_row)]
    row_copies = [
        copy(summed.at[k], row_landed.at[k], n_row + k, (row_at(k), col)) for k in range(1, n_row)
    ]
    chip_copies = [
        copy(second.at[chip_at(k)], chip_landed.at[k], 2 * n_row + k, (row, chip_at(k) * 2 + core))
        for k in range(1, chips)
    ]
    order = list(range(1, n_row)) + [0]
    for k in order:
        swaps[k].start()
    for k in order:
        swaps[k].wait()
        summed[k] = x_ref[core, row_at(k)] + pair[k]
        if k > 0:
            row_copies[k - 1].start()
    total = summed[0]
    for k in range(1, n_row):
        row_copies[k - 1].wait()
        total = total + row_landed[k]
    second[...] = total
    for c in chip_copies:
        c.start()
    result = second[chip]
    for k in range(1, chips):
        chip_copies[k - 1].wait()
        result = result + chip_landed[k]
    out_ref[...] = result


def reduce_numer(n_row, n_col, x):
    lines, span = x.shape[3:]
    chips = n_col // 2
    return pl.pallas_call(
        functools.partial(reduce_kernel, n_row, n_col),
        in_specs=[pl.BlockSpec(memory_space=pltpu.VMEM)],
        out_specs=pl.BlockSpec(memory_space=pltpu.VMEM),
        out_shape=jax.ShapeDtypeStruct((lines, span), jnp.float32),
        scratch_shapes=[
            pltpu.VMEM((n_row, chips, lines, span), x.dtype),
            pltpu.VMEM((n_row, chips, lines, span), x.dtype),
            pltpu.VMEM((n_row, chips, lines, span), x.dtype),
            pltpu.VMEM((chips, lines, span), x.dtype),
            pltpu.VMEM((chips, lines, span), x.dtype),
            pltpu.SemaphoreType.DMA((2 * n_row + chips,)),
            pltpu.SemaphoreType.DMA((2 * n_row + chips,)),
        ],
        compiler_params=pltpu.CompilerParams(collective_id=4, has_side_effects=True),
        name="reduce_numer",
    )(x)


def energy_kernel(
    frames, group, n_row, n_col, x_ref, table_ref, h_ref, out_ref, h_all_ref, scratch, held, sends, recvs
):
    step = pl.program_id(0)
    gather = Gather(n_row, n_col, held, sends, recvs)

    @pl.when(step == 0)
    def _():
        gather.place(h_ref)
        greet(gather.partners())

    for number in range(4):

        @pl.when(step == 2 * number + 1)
        def _():
            gather.stage(number)

    @pl.when(step == 7)
    def _():
        h_all_ref[...] = held[...]

    channels = x_ref.shape[0]
    table = table_ref[...]
    for first in range(0, frames, group):
        lhs = jnp.concatenate(
            [x_ref[:, f * WIN : (f + 1) * WIN] for f in range(first, first + group)], axis=0
        )
        spectrum = jnp.dot(lhs, table, preferred_element_type=jnp.float32)
        real_part = spectrum[:, :BINS]
        imag_part = spectrum[:, BINS:]
        scratch[pl.ds(first * channels, group * channels), :] = (
            real_part * real_part + imag_part * imag_part
        )
    for ch in range(channels):
        out_ref[ch] = scratch[pl.ds(ch, frames, stride=channels), :].astype(jnp.bfloat16)


def frame_energy(n_row, n_col, record, table, h_b):
    channels, samples = record.shape
    frames = samples // WIN
    block = 32
    assert channels // block >= 8
    return pl.pallas_call(
        functools.partial(energy_kernel, frames, 16, n_row, n_col),
        grid=(channels // block,),
        in_specs=[
            pl.BlockSpec((block, samples), lambda i: (i, 0)),
            pl.BlockSpec((WIN, 2 * BINS), lambda i: (0, 0)),
            pl.BlockSpec(memory_space=pltpu.VMEM),
        ],
        out_specs=[
            pl.BlockSpec((block, frames, BINS), lambda i: (i, 0, 0)),
            pl.BlockSpec(memory_space=pltpu.VMEM),
        ],
        out_shape=[
            jax.ShapeDtypeStruct((channels, frames, BINS), jnp.bfloat16),
            jax.ShapeDtypeStruct((n_row, 2, n_col // 2, *h_b.shape), h_b.dtype),
        ],
        scratch_shapes=[pltpu.VMEM((frames * block, BINS), jnp.float32)]
        + gather_scratch(n_row, n_col, h_b),
        compiler_params=pltpu.CompilerParams(collective_id=1, has_side_effects=True),
        name="frame_energy",
    )(record, table, h_b)


def sweep_kernel(spectra_ref, w_ref, h_ref, numer_ref, w_out_ref, w_b, wt_b, wn_t, rowsum, colsum):
    step = pl.program_id(0)
    n_row, _, chans, frames, bins = spectra_ref.shape
    ranks = h_ref.shape[3]

    @pl.when(step == 0)
    def _():
        w_b[...] = w_ref[...].astype(jnp.bfloat16)
        wt_b[...] = w_ref[...].T.astype(jnp.bfloat16)
        wn_t[...] = jnp.zeros_like(wn_t)
        colsum[...] = jnp.zeros_like(colsum)
        rowsum[...] = jnp.zeros_like(rowsum)
        total = jnp.sum(w_b[...].astype(jnp.float32), axis=0, keepdims=True)
        line = lax.broadcasted_iota(jnp.int32, (colsum.shape[0], total.shape[1]), 0)
        colsum[:, : total.shape[1]] = jnp.where(line == 0, total, 0.0)

    h_b = jnp.concatenate([h_ref[r, 0, 0] for r in range(n_row)], axis=0)
    h_f = h_b.astype(jnp.float32)
    rowsum[...] += jnp.sum(h_f, axis=1, keepdims=True)
    ht_b = h_f.T.astype(jnp.bfloat16)
    recon = jnp.dot(ht_b, wt_b[...], preferred_element_type=jnp.float32)
    tile = jnp.concatenate(
        [
            jnp.concatenate([spectra_ref[r, 0, c] for c in range(chans)], axis=1)
            for r in range(n_row)
        ],
        axis=0,
    )
    quotient = (tile.astype(jnp.float32) / recon).astype(jnp.bfloat16)
    hn = jnp.dot(quotient, w_b[...], preferred_element_type=jnp.float32).T
    wn_t[...] += jnp.dot(h_b, quotient, preferred_element_type=jnp.float32)
    for r in range(n_row):
        numer_ref[0, r, 0, :ranks, :] = hn[r * ranks : (r + 1) * ranks]
        numer_ref[0, r, 0, ranks:, :] = colsum[...]

    @pl.when(step == pl.num_programs(0) - 1)
    def _():
        w_out_ref[...] = w_ref[...] * (wn_t[...] / rowsum[...]).T


def sweep_terms(spectra, w_state, h_all):
    n_row, n_col, chans, frames, bins = spectra.shape
    rows, rank = w_state.shape
    ranks, span = h_all.shape[3:]
    lines = ranks + 8
    assert span >= rank
    return pl.pallas_call(
        sweep_kernel,
        grid=(n_col,),
        in_specs=[
            pl.BlockSpec((n_row, 1, chans, frames, bins), lambda i: (0, i, 0, 0, 0)),
            pl.BlockSpec((rows, rank), lambda i: (0, 0)),
            pl.BlockSpec((n_row, 1, 1, ranks, span), lambda i: (0, i % 2, i // 2, 0, 0)),
        ],
        out_specs=[
            pl.BlockSpec((1, n_row, 1, lines, span), lambda i: (i % 2, 0, i // 2, 0, 0)),
            pl.BlockSpec((rows, rank), lambda i: (0, 0)),
        ],
        out_shape=[
            jax.ShapeDtypeStruct((2, n_row, n_col // 2, lines, span), jnp.float32),
            jax.ShapeDtypeStruct((rows, rank), jnp.float32),
        ],
        scratch_shapes=[
            pltpu.VMEM((rows, rank), jnp.bfloat16),
            pltpu.VMEM((rank, rows), jnp.bfloat16),
            pltpu.VMEM((rank, rows), jnp.float32),
            pltpu.VMEM((rank, 1), jnp.float32),
            pltpu.VMEM((8, span), jnp.float32),
        ],
        name="sweep_terms",
    )(spectra, w_state, h_all)


def local(n_row, n_col, samples, w_start, h_start):
    n = n_row * n_col
    table = dft_table()
    record = samples.reshape(samples.shape[2], samples.shape[3])
    energy, h_all = frame_energy(n_row, n_col, record, table, h_start.astype(jnp.bfloat16))
    channels, frames, bins = energy.shape
    energy = energy.reshape(n, channels // n, frames, bins)
    spectra = exchange(n_row, n_col, energy, pl.ANY, 3, "exchange_spectra")
    spectra = spectra.reshape(n_row, n_col, channels // n, frames, bins)
    ranks, span = h_start.shape
    rank = w_start.shape[1]
    w_state = w_start
    h_state = h_start
    first = lax.axis_index("row") * ranks
    for sweep in range(ITERS):
        if sweep > 0:
            h_all = gather_factor(n_row, n_col, h_state.astype(jnp.bfloat16))
        numer, w_state = sweep_terms(spectra, w_state, h_all)
        total = reduce_numer(n_row, n_col, numer)
        colsum = total[ranks, :rank]
        colsum = lax.dynamic_slice(colsum, (first,), (ranks,))
        h_state = h_state * total[:ranks] / colsum[:, None]
    return (w_state, h_state)


def solution(mesh):
    placed = (P("col", "row", None, None), P(("row", "col"), None), P("row", "col"))
    return jax.shard_map(
        functools.partial(local, mesh.shape["row"], mesh.shape["col"]),
        mesh=mesh,
        in_specs=placed,
        out_specs=(P(("row", "col"), None), P("row", "col")),
        check_vma=False,
    )
```

```python
import functools
import math

import jax
import jax.numpy as jnp
from jax import lax
from jax.experimental import pallas as pl
from jax.experimental.pallas import tpu as pltpu
from jax.sharding import PartitionSpec as P

BINS = 128
ITERS = 2
WIN = 256


def dft_table():
    sample_idx = jnp.arange(WIN, dtype=jnp.int32)
    bin_idx = jnp.arange(BINS, dtype=jnp.int32)
    phases = sample_idx[:, None] * bin_idx[None, :] % WIN
    phases = phases.astype(jnp.float32) * (2.0 * math.pi / WIN)
    shaping = 0.5 - 0.5 * jnp.cos(sample_idx.astype(jnp.float32) * (2.0 * math.pi / WIN))
    shaping = shaping / math.sqrt(3.0 * WIN / 8.0)
    both = jnp.concatenate(
        [shaping[:, None] * jnp.cos(phases), -shaping[:, None] * jnp.sin(phases)], axis=1
    )
    return both.astype(jnp.bfloat16)


MESH = pl.DeviceIdType.MESH


def greet(partners):
    barrier = pltpu.get_barrier_semaphore()
    for row, col in partners:
        pl.semaphore_signal(barrier, inc=1, device_id={"row": row, "col": col}, device_id_type=MESH)
    pl.semaphore_wait(barrier, len(partners))


class Gather:
    def __init__(self, n_row, n_col, out, sends, recvs):
        self.n_row, self.n_col = n_row, n_col
        self.row, self.col = lax.axis_index("row"), lax.axis_index("col")
        self.core, self.chip = lax.rem(self.col, 2), self.col // 2
        self.chips = n_col // 2
        self.out, self.sends, self.recvs = out, sends, recvs

    def chip_partner(self, k):
        return self.row, lax.rem(self.chip + k, self.chips) * 2 + self.core

    def row_partner(self, k):
        return lax.rem(self.row + k, self.n_row), self.col

    def core_partner(self):
        return self.row, self.chip * 2 + 1 - self.core

    def partners(self):
        chips = [self.chip_partner(k) for k in range(1, self.chips)]
        rows = [self.row_partner(k) for k in range(1, self.n_row)]
        return chips + rows + [self.core_partner()]

    def copy(self, src, dst, index, partner):
        return pltpu.make_async_remote_copy(
            src_ref=src,
            dst_ref=dst,
            send_sem=self.sends.at[index],
            recv_sem=self.recvs.at[index],
            device_id={"row": partner[0], "col": partner[1]},
            device_id_type=MESH,
        )

    def chip_copies(self):
        slot = self.out.at[self.row, self.core, self.chip]
        return [self.copy(slot, slot, k - 1, self.chip_partner(k)) for k in range(1, self.chips)]

    def row_copies(self):
        slot = self.out.at[self.row, self.core]
        base = self.chips - 2
        return [self.copy(slot, slot, base + k, self.row_partner(k)) for k in range(1, self.n_row)]

    def core_copies(self):
        base = self.chips + self.n_row - 2
        slots = [self.out.at[r, self.core] for r in range(self.n_row)]
        return [self.copy(s, s, base + r, self.core_partner()) for r, s in enumerate(slots)]

    def place(self, mine):
        self.out[self.row, self.core, self.chip] = mine[...]

    def stage(self, number):
        lists = (self.chip_copies, self.row_copies, self.core_copies)
        if number > 0:
            for copy in lists[number - 1]():
                copy.wait()
        if number < 3:
            for copy in lists[number]():
                copy.start()


def gather_scratch(n_row, n_col, h_b):
    sems = pltpu.SemaphoreType.DMA((n_col // 2 + 2 * n_row,))
    return [pltpu.VMEM((n_row, 2, n_col // 2, *h_b.shape), h_b.dtype), sems, sems]


def gather_kernel(n_row, n_col, h_ref, out_ref, held, sends, recvs):
    gather = Gather(n_row, n_col, held, sends, recvs)
    gather.place(h_ref)
    greet(gather.partners())
    for number in range(4):
        gather.stage(number)
    out_ref[...] = held[...]


def gather_factor(n_row, n_col, h_b):
    return pl.pallas_call(
        functools.partial(gather_kernel, n_row, n_col),
        in_specs=[pl.BlockSpec(memory_space=pltpu.VMEM)],
        out_specs=pl.BlockSpec(memory_space=pltpu.VMEM),
        out_shape=jax.ShapeDtypeStruct((n_row, 2, n_col // 2, *h_b.shape), h_b.dtype),
        scratch_shapes=gather_scratch(n_row, n_col, h_b),
        compiler_params=pltpu.CompilerParams(collective_id=2, has_side_effects=True),
        name="gather_factor",
    )(h_b)


def reduce_kernel(
    n_row, n_col, x_ref, out_ref, pair, summed, row_landed, second, chip_landed, sends, recvs
):
    row, col = lax.axis_index("row"), lax.axis_index("col")
    core, chip = lax.rem(col, 2), col // 2
    chips = n_col // 2

    def row_at(k):
        return lax.rem(row + k, n_row)

    def chip_at(k):
        return lax.rem(chip + k, chips)

    mate = (row, chip * 2 + 1 - core)
    greet(
        [mate]
        + [(row_at(k), col) for k in range(1, n_row)]
        + [(row, chip_at(k) * 2 + core) for k in range(1, chips)]
    )

    def copy(src, dst, index, partner):
        return pltpu.make_async_remote_copy(
            src_ref=src,
            dst_ref=dst,
            send_sem=sends.at[index],
            recv_sem=recvs.at[index],
            device_id={"row": partner[0], "col": partner[1]},
            device_id_type=MESH,
        )

    swaps = [copy(x_ref.at[1 - core, row_at(k)], pair.at[k], k, mate) for k in range(n_row)]
    row_copies = [
        copy(summed.at[k], row_landed.at[k], n_row + k, (row_at(k), col)) for k in range(1, n_row)
    ]
    chip_copies = [
        copy(second.at[chip_at(k)], chip_landed.at[k], 2 * n_row + k, (row, chip_at(k) * 2 + core))
        for k in range(1, chips)
    ]
    order = list(range(1, n_row)) + [0]
    for k in order:
        swaps[k].start()
    for k in order:
        swaps[k].wait()
        summed[k] = x_ref[core, row_at(k)] + pair[k]
        if k > 0:
            row_copies[k - 1].start()
    total = summed[0]
    for k in range(1, n_row):
        row_copies[k - 1].wait()
        total = total + row_landed[k]
    second[...] = total
    for c in chip_copies:
        c.start()
    result = second[chip]
    for k in range(1, chips):
        chip_copies[k - 1].wait()
        result = result + chip_landed[k]
    out_ref[...] = result


def reduce_numer(n_row, n_col, x):
    lines, span = x.shape[3:]
    chips = n_col // 2
    return pl.pallas_call(
        functools.partial(reduce_kernel, n_row, n_col),
        in_specs=[pl.BlockSpec(memory_space=pltpu.VMEM)],
        out_specs=pl.BlockSpec(memory_space=pltpu.VMEM),
        out_shape=jax.ShapeDtypeStruct((lines, span), jnp.float32),
        scratch_shapes=[
            pltpu.VMEM((n_row, chips, lines, span), x.dtype),
            pltpu.VMEM((n_row, chips, lines, span), x.dtype),
            pltpu.VMEM((n_row, chips, lines, span), x.dtype),
            pltpu.VMEM((chips, lines, span), x.dtype),
            pltpu.VMEM((chips, lines, span), x.dtype),
            pltpu.SemaphoreType.DMA((2 * n_row + chips,)),
            pltpu.SemaphoreType.DMA((2 * n_row + chips,)),
        ],
        compiler_params=pltpu.CompilerParams(collective_id=4, has_side_effects=True),
        name="reduce_numer",
    )(x)


def first_block(n_row, n_col, blocks):
    me = lax.axis_index("row") * n_col + lax.axis_index("col")
    return me * blocks // (n_row * n_col)


def energy_kernel(
    frames,
    group,
    n_row,
    n_col,
    x_ref,
    table_ref,
    h_ref,
    out_ref,
    h_all_ref,
    scratch,
    energy,
    block_sends,
    block_recvs,
    own_sem,
    held,
    sends,
    recvs,
):
    step, steps = pl.program_id(0), pl.num_programs(0)
    gather = Gather(n_row, n_col, held, sends, recvs)
    n = n_row * n_col
    row, col = lax.axis_index("row"), lax.axis_index("col")
    me = row * n_col + col
    channels = x_ref.shape[0]
    chans = out_ref.shape[1]
    per = channels // chans
    start_block = first_block(n_row, n_col, n // per)

    def block_copy(target):
        shift = lax.rem(target - me + n, n)
        return pltpu.make_async_remote_copy(
            src_ref=energy.at[pl.ds(target * chans, chans)],
            dst_ref=out_ref.at[me],
            send_sem=block_sends.at[shift],
            recv_sem=block_recvs.at[shift],
            device_id={"row": target // n_col, "col": lax.rem(target, n_col)},
            device_id_type=MESH,
        )

    def own_copy():
        return pltpu.make_async_copy(
            energy.at[pl.ds(me * chans, chans)], out_ref.at[me], own_sem
        )

    def send_block(number):
        base = lax.rem(start_block + number, n // per) * per

        def send(j, carry):
            target = base + lax.rem(j + me, per)

            @pl.when(target != me)
            def _():
                block_copy(target).start()

            @pl.when(target == me)
            def _():
                own_copy().start()

            return carry

        lax.fori_loop(0, per, send, 0)

    @pl.when(step == 0)
    def _():
        barrier = pltpu.get_barrier_semaphore()
        gather.place(h_ref)

        def signal(k, carry):
            target = lax.rem(me + k, n)
            pl.semaphore_signal(
                barrier,
                inc=1,
                device_id={"row": target // n_col, "col": lax.rem(target, n_col)},
                device_id_type=MESH,
            )
            return carry

        lax.fori_loop(1, n, signal, 0)
        pl.semaphore_wait(barrier, n - 1)
        gather.stage(0)

    @pl.when(step == 1)
    def _():
        gather.stage(1)

    @pl.when(step == 4)
    def _():
        gather.stage(2)

    @pl.when(step >= 1)
    def _():
        send_block(step - 1)

    table = table_ref[...]
    for first in range(0, frames, group):
        lhs = jnp.concatenate(
            [x_ref[:, f * WIN : (f + 1) * WIN] for f in range(first, first + group)], axis=0
        )
        spectrum = jnp.dot(lhs, table, preferred_element_type=jnp.float32)
        real_part = spectrum[:, :BINS]
        imag_part = spectrum[:, BINS:]
        scratch[pl.ds(first * channels, group * channels), :] = (
            real_part * real_part + imag_part * imag_part
        )
    base_channel = lax.rem(start_block + step, n // per) * channels
    for ch in range(channels):
        energy[base_channel + ch] = scratch[pl.ds(ch, frames, stride=channels), :].astype(
            jnp.bfloat16
        )

    @pl.when(step == steps - 1)
    def _():
        send_block(step)
        gather.stage(3)
        h_all_ref[...] = held[...]

        def finish(k, carry):
            block_copy(lax.rem(me + k, n)).wait()
            return carry

        lax.fori_loop(1, n, finish, 0)
        own_copy().wait()


def frame_energy(n_row, n_col, record, table, h_b):
    channels, samples = record.shape
    frames = samples // WIN
    block = 32
    n = n_row * n_col
    blocks = channels // block
    assert blocks >= 6 and n % blocks == 0
    return pl.pallas_call(
        functools.partial(energy_kernel, frames, 16, n_row, n_col),
        grid=(blocks,),
        in_specs=[
            pl.BlockSpec(
                (block, samples),
                lambda i: (lax.rem(first_block(n_row, n_col, blocks) + i, blocks), 0),
            ),
            pl.BlockSpec((WIN, 2 * BINS), lambda i: (0, 0)),
            pl.BlockSpec(memory_space=pltpu.VMEM),
        ],
        out_specs=[
            pl.BlockSpec(memory_space=pl.ANY),
            pl.BlockSpec(memory_space=pltpu.VMEM),
        ],
        out_shape=[
            jax.ShapeDtypeStruct((n, channels // n, frames, BINS), jnp.bfloat16),
            jax.ShapeDtypeStruct((n_row, 2, n_col // 2, *h_b.shape), h_b.dtype),
        ],
        scratch_shapes=[
            pltpu.VMEM((frames * block, BINS), jnp.float32),
            pltpu.VMEM((channels, frames, BINS), jnp.bfloat16),
            pltpu.SemaphoreType.DMA((n,)),
            pltpu.SemaphoreType.DMA((n,)),
            pltpu.SemaphoreType.DMA,
        ]
        + gather_scratch(n_row, n_col, h_b),
        compiler_params=pltpu.CompilerParams(collective_id=1, has_side_effects=True),
        name="frame_energy",
    )(record, table, h_b)


def sweep_kernel(spectra_ref, w_ref, h_ref, numer_ref, w_out_ref, w_b, wt_b, wn_t, rowsum, colsum):
    step = pl.program_id(0)
    n_row, _, chans, frames, bins = spectra_ref.shape
    ranks = h_ref.shape[3]

    @pl.when(step == 0)
    def _():
        w_b[...] = w_ref[...].astype(jnp.bfloat16)
        wt_b[...] = w_ref[...].T.astype(jnp.bfloat16)
        wn_t[...] = jnp.zeros_like(wn_t)
        colsum[...] = jnp.zeros_like(colsum)
        rowsum[...] = jnp.zeros_like(rowsum)
        total = jnp.sum(w_b[...].astype(jnp.float32), axis=0, keepdims=True)
        line = lax.broadcasted_iota(jnp.int32, (colsum.shape[0], total.shape[1]), 0)
        colsum[:, : total.shape[1]] = jnp.where(line == 0, total, 0.0)

    h_b = jnp.concatenate([h_ref[r, 0, 0] for r in range(n_row)], axis=0)
    h_f = h_b.astype(jnp.float32)
    rowsum[...] += jnp.sum(h_f, axis=1, keepdims=True)
    ht_b = h_f.T.astype(jnp.bfloat16)
    recon = jnp.dot(ht_b, wt_b[...], preferred_element_type=jnp.float32)
    tile = jnp.concatenate(
        [
            jnp.concatenate([spectra_ref[r, 0, c] for c in range(chans)], axis=1)
            for r in range(n_row)
        ],
        axis=0,
    )
    quotient = (tile.astype(jnp.float32) / recon).astype(jnp.bfloat16)
    hn = jnp.dot(quotient, w_b[...], preferred_element_type=jnp.float32).T
    wn_t[...] += jnp.dot(h_b, quotient, preferred_element_type=jnp.float32)
    for r in range(n_row):
        numer_ref[0, r, 0, :ranks, :] = hn[r * ranks : (r + 1) * ranks]
        numer_ref[0, r, 0, ranks:, :] = colsum[...]

    @pl.when(step == pl.num_programs(0) - 1)
    def _():
        w_out_ref[...] = w_ref[...] * (wn_t[...] / rowsum[...]).T


def sweep_terms(spectra, w_state, h_all):
    n_row, n_col, chans, frames, bins = spectra.shape
    rows, rank = w_state.shape
    ranks, span = h_all.shape[3:]
    lines = ranks + 8
    assert span >= rank
    return pl.pallas_call(
        sweep_kernel,
        grid=(n_col,),
        in_specs=[
            pl.BlockSpec((n_row, 1, chans, frames, bins), lambda i: (0, i, 0, 0, 0)),
            pl.BlockSpec((rows, rank), lambda i: (0, 0)),
            pl.BlockSpec((n_row, 1, 1, ranks, span), lambda i: (0, i % 2, i // 2, 0, 0)),
        ],
        out_specs=[
            pl.BlockSpec((1, n_row, 1, lines, span), lambda i: (i % 2, 0, i // 2, 0, 0)),
            pl.BlockSpec((rows, rank), lambda i: (0, 0)),
        ],
        out_shape=[
            jax.ShapeDtypeStruct((2, n_row, n_col // 2, lines, span), jnp.float32),
            jax.ShapeDtypeStruct((rows, rank), jnp.float32),
        ],
        scratch_shapes=[
            pltpu.VMEM((rows, rank), jnp.bfloat16),
            pltpu.VMEM((rank, rows), jnp.bfloat16),
            pltpu.VMEM((rank, rows), jnp.float32),
            pltpu.VMEM((rank, 1), jnp.float32),
            pltpu.VMEM((8, span), jnp.float32),
        ],
        name="sweep_terms",
    )(spectra, w_state, h_all)


def local(n_row, n_col, samples, w_start, h_start):
    table = dft_table()
    record = samples.reshape(samples.shape[2], samples.shape[3])
    spectra, h_all = frame_energy(n_row, n_col, record, table, h_start.astype(jnp.bfloat16))
    n, chans, frames, bins = spectra.shape
    spectra = spectra.reshape(n_row, n_col, chans, frames, bins)
    ranks, span = h_start.shape
    rank = w_start.shape[1]
    w_state = w_start
    h_state = h_start
    first = lax.axis_index("row") * ranks
    for sweep in range(ITERS):
        if sweep > 0:
            h_all = gather_factor(n_row, n_col, h_state.astype(jnp.bfloat16))
        numer, w_state = sweep_terms(spectra, w_state, h_all)
        total = reduce_numer(n_row, n_col, numer)
        colsum = total[ranks, :rank]
        colsum = lax.dynamic_slice(colsum, (first,), (ranks,))
        h_state = h_state * total[:ranks] / colsum[:, None]
    return (w_state, h_state)


def solution(mesh):
    placed = (P("col", "row", None, None), P(("row", "col"), None), P("row", "col"))
    return jax.shard_map(
        functools.partial(local, mesh.shape["row"], mesh.shape["col"]),
        mesh=mesh,
        in_specs=placed,
        out_specs=(P(("row", "col"), None), P("row", "col")),
        check_vma=False,
    )
```
